8 devices in a mesh: data: 1 (over z), pp: 2 (over y), ep: 4 (over x, core).
Axes of the slice: x: 2, y: 2, z: 1, core: 2. Of those that a mesh axis runs over, the one named last changes fastest.
Arguments:
- O: bfloat16 [2, 8, 8, 640, 4096], P(('data', 'pp'), None, 'ep')
- idx: int32 [2, 8, 4, 512, 2], P(('data', 'pp'), None, 'ep')
- slot: int32 [2, 8, 4, 512, 2], P(('data', 'pp'), None, 'ep')
- g: float32 [2, 8, 4, 512, 2], P(('data', 'pp'), None, 'ep')
- H: bfloat16 [2, 8, 4, 512, 4096], P(('data', 'pp'), None, 'ep')
- w: float32 [2, 4096], P('pp')
- Wq: bfloat16 [2, 4096, 32, 128], P('pp')
- Wk: bfloat16 [2, 4096, 32, 128], P('pp')
- Wv: bfloat16 [2, 4096, 32, 128], P('pp')
- Wo: bfloat16 [2, 32, 128, 4096], P('pp')
Outputs:
- output: bfloat16 [2, 8, 4, 512, 4096], P(('data', 'pp'), None, 'ep')
All inputs are finite; a program needn't handle non-finite values.
Results may differ from the reference program's by a relative error of at most 0.00686826.
Values are sent between devices in bfloat16 or wider.
A program may use at most 1.25 GiB of HBM per device.

```python
import math
import jax
import jax.numpy as jnp
from jax import lax

PP = 2
EP = 4
M = 8
SEQ_DEV = 1
L = 512
D = 4096
HEADS = 32
HEAD_DIM = 128
EXPERTS = 8
TOP = 2
CG = 160

EPS = 1e-6
SEQS = EP * SEQ_DEV
TD = SEQ_DEV * L
T = EP * TD
C = EP * CG
QKV = HEADS * HEAD_DIM


def ranks(e, pr):
    n = e.shape[0]
    order = jnp.argsort(e * n + pr)
    se = e[order]
    start = jnp.searchsorted(se, se, side='left').astype(jnp.int32)
    r = jnp.arange(n, dtype=jnp.int32) - start
    return jnp.zeros((n,), jnp.int32).at[order].set(r)


def setup_inputs(seed: int = 0, part: int = 0) -> dict:
    ks = jax.random.split(jax.random.fold_in(jax.random.key(seed), part), 8)
    kd = jax.random.split(jax.random.fold_in(jax.random.fold_in(jax.random.key(seed), part), 7), 3)
    kw = jax.random.split(jax.random.key(seed + 1), 5)
    normal_sum = jnp.sum(jax.random.randint(kd[0], (PP, 4, EXPERTS), 0, 256), axis=1)
    octave_step = ((4 * 255 - normal_sum) // 16).astype(jnp.uint32)
    mant_table = jnp.array([256, 279, 304, 332, 362, 395, 431, 470], dtype=jnp.uint32)
    inv_weight = jnp.repeat(mant_table[octave_step & 7] << (octave_step >> 3), M, axis=0)

    def route(i):
        raw_bits = jax.random.bits(jax.random.fold_in(kd[1], i), (T, EXPERTS), jnp.uint32) >> 16
        wait_time = raw_bits * inv_weight[i]
        return jnp.argsort(wait_time, axis=-1)[:, :TOP].astype(jnp.int32)

    idx = lax.map(route, jnp.arange(PP * M))
    n = TD * TOP
    prio = jnp.argsort(jax.random.uniform(kd[2], (PP * M * EP, n)), axis=-1).astype(jnp.int32)
    r = jax.vmap(ranks)(idx.reshape(PP * M * EP, n), prio).reshape(PP * M, EP, TD, TOP)
    first = (jnp.arange(EP, dtype=jnp.int32) * CG)[None, :, None, None]
    slot = jnp.where(r < CG, r + first, -1).reshape(PP, M, SEQS, L, TOP)
    idx = idx.reshape(PP, M, SEQS, L, TOP)
    g = jax.nn.softmax(1.2 * jax.random.normal(ks[2], (PP, M, SEQS, L, TOP)), axis=-1)
    scale = jnp.exp(0.5 * jax.random.normal(ks[3], (PP, 1, EXPERTS, 1, 1)))
    mu = jax.random.normal(ks[4], (PP, 1, EXPERTS, 1, D))
    O = (scale * (jax.random.normal(ks[5], (PP, M, EXPERTS, C, D)) + 0.8 * mu)).astype(jnp.bfloat16)
    H = jax.random.normal(ks[6], (PP, M, SEQS, L, D)).astype(jnp.bfloat16)
    w = 1.0 + 0.4 * jax.random.normal(kw[0], (PP, D))
    sharp = (0.75 * math.log(L)) ** 0.25 / math.sqrt(D)
    Wq = (sharp * jax.random.normal(kw[1], (PP, D, HEADS, HEAD_DIM))).astype(jnp.bfloat16)
    Wk = (sharp * jax.random.normal(kw[2], (PP, D, HEADS, HEAD_DIM))).astype(jnp.bfloat16)
    Wv = (jax.random.normal(kw[3], (PP, D, HEADS, HEAD_DIM)) / math.sqrt(D)).astype(jnp.bfloat16)
    Wo = (jax.random.normal(kw[4], (PP, HEADS, HEAD_DIM, D)) / math.sqrt(QKV)).astype(jnp.bfloat16)
    return dict(O=O, idx=idx, slot=slot, g=g.astype(jnp.float32), H=H, w=w.astype(jnp.float32), Wq=Wq, Wk=Wk, Wv=Wv, Wo=Wo)


def combine(o, ix, sl, gt, h):
    flat = o.reshape(EXPERTS * C, D)
    acc = h.astype(jnp.float32)
    for kk in range(TOP):
        s = sl[:, kk]
        valid = s >= 0
        rows = jnp.take(flat, ix[:, kk] * C + jnp.where(valid, s, 0), axis=0)
        acc = acc + jnp.where(valid, gt[:, kk], 0.0)[:, None] * rows.astype(jnp.float32)
    return acc.astype(jnp.bfloat16)


def head_attn(a):
    qh, kh, vh = a
    s = jnp.dot(qh, kh.T, preferred_element_type=jnp.float32) * (HEAD_DIM ** -0.5)
    r = lax.broadcasted_iota(jnp.int32, (L, L), 0)
    c = lax.broadcasted_iota(jnp.int32, (L, L), 1)
    p = jax.nn.softmax(jnp.where(r >= c, s, -1e30), axis=-1)
    return jnp.dot(p, vh.astype(jnp.float32))


def layer(y, wn, wq, wk, wv, wo):
    yf = y.astype(jnp.float32)
    x = (yf * lax.rsqrt(jnp.mean(yf * yf, axis=-1, keepdims=True) + EPS) * wn).astype(jnp.bfloat16)
    q = jnp.dot(x, wq.reshape(D, QKV), preferred_element_type=jnp.float32).astype(jnp.bfloat16)
    k = jnp.dot(x, wk.reshape(D, QKV), preferred_element_type=jnp.float32).astype(jnp.bfloat16)
    v = jnp.dot(x, wv.reshape(D, QKV), preferred_element_type=jnp.float32).astype(jnp.bfloat16)

    def heads(t):
        return t.reshape(SEQS, L, HEADS, HEAD_DIM).transpose(0, 2, 1, 3).reshape(SEQS * HEADS, L, HEAD_DIM)

    o = lax.map(head_attn, (heads(q), heads(k), heads(v)))
    o = o.reshape(SEQS, HEADS, L, HEAD_DIM).transpose(0, 2, 1, 3).reshape(T, QKV).astype(jnp.bfloat16)
    a = jnp.dot(o, wo.reshape(QKV, D), preferred_element_type=jnp.float32).astype(jnp.bfloat16)
    return (yf + a.astype(jnp.float32)).astype(jnp.bfloat16)


def reference(O, idx, slot, g, H, w, Wq, Wk, Wv, Wo):
    y = lax.map(lambda a: combine(a[0], a[1], a[2], a[3], a[4]),
                (O.reshape(PP * M, EXPERTS, C, D), idx.reshape(PP * M, T, TOP), slot.reshape(PP * M, T, TOP),
                 g.reshape(PP * M, T, TOP), H.reshape(PP * M, T, D)))
    y = jnp.roll(y.reshape(PP, M, T, D), 1, axis=0)

    def stage(a):
        ys, wn, wq, wk, wv, wo = a
        return lax.map(lambda yy: layer(yy, wn, wq, wk, wv, wo), ys)

    z = lax.map(stage, (y, w, Wq, Wk, Wv, Wo))
    return z.reshape(PP, M, SEQS, L, D)
```

```python
import functools
import math

import jax
import jax.numpy as jnp
from jax import lax
from jax.experimental import pallas as pl
from jax.experimental.pallas import tpu as pltpu
from jax.sharding import PartitionSpec as P


EPS = 1e-6
HD = 128
F32 = jnp.float32
BF16 = jnp.bfloat16
VMEM_LIMIT = 63 * 1024 * 1024
ANY = pl.BlockSpec(memory_space=pl.ANY)
TOK = jax.ShapeDtypeStruct((8, 128), F32)


def cost(flops):
    return pl.CostEstimate(flops=int(flops), bytes_accessed=int(flops) // 256, transcendentals=0)


def slice_kernel(rows_ref, tok, o_ref, out_ref, tok_out):
    out_ref[...] = o_ref[...].reshape(out_ref.shape)


def slice_rows(rows, tok, o, m0, nm, cg):
    _, ne, _, d = o.shape
    n_own = rows.shape[0]
    return pl.pallas_call(
        slice_kernel,
        grid_spec=pltpu.PrefetchScalarGridSpec(
            num_scalar_prefetch=1,
            grid=(nm, n_own),
            in_specs=[ANY, pl.BlockSpec((1, ne, cg, d), lambda m, a, r: (m0 + m, 0, r[a], 0))],
            out_specs=[pl.BlockSpec((1, 1, ne, cg, d), lambda m, a, r: (m, a, 0, 0, 0)), ANY],
        ),
        out_shape=[jax.ShapeDtypeStruct((nm, n_own, ne, cg, d), o.dtype), TOK],
        input_output_aliases={1: 1},
        compiler_params=pltpu.CompilerParams(vmem_limit_bytes=VMEM_LIMIT),
        cost_estimate=cost(nm * 2e9),
        name="slice_rows",
    )(rows, tok, o)


CW = 1024
AHEAD = 2
FAR, NEAR = 1, 0


def pack_kernel(jobs, ne, cg, nep, n, *refs):
    nj = len(jobs)
    nsib = 1 + max(job[4] for job in jobs)
    o = refs[1]
    sibs, tabs = refs[2:2 + nsib], refs[2 + nsib:4 + nsib]
    outs = refs[4 + nsib:4 + nsib + nj]
    _, in_s, out_s, sel_ref, tab_ref, isem, osem, tsem = refs[4 + nsib + nj:]
    j = lax.axis_index('ep')
    firsts = (j * cg, lax.rem(j + nep // 2, nep) * cg)

    def fetch(i, c, slot):
        m, which, _, _, s, ms = jobs[i]
        cs = pl.ds(pl.multiple_of(c * CW, CW), CW)
        rs = pl.ds(pl.multiple_of(firsts[which], 16), cg)
        src = [o.at[m, e, rs, cs] for e in range(ne)]
        src += [sibs[s].at[ms, which, e, :, cs] for e in range(ne)]
        return [pltpu.make_async_copy(v, in_s.at[slot, pl.ds(e * cg, cg)], isem.at[slot, e]) for e, v in enumerate(src)]

    def put(i, c, slot):
        ls = pl.ds(pl.multiple_of(c * CW, CW), CW)
        return pltpu.make_async_copy(out_s.at[slot, pl.ds(0, jobs[i][3])], outs[i].at[:, ls], osem.at[slot])

    def at(i, c, f):
        for k, lo in ((i - 1, -n), (i, 0), (i + 1, n)):
            if 0 <= k < nj:
                @pl.when(jnp.logical_and(c >= lo, c < lo + n))
                def _():
                    f(k, c - lo, i * n + c)

    tables = [pltpu.make_async_copy(t, tab_ref.at[k], tsem.at[k]) for k, t in enumerate(tabs)]
    for t in tables:
        t.start()
    for t in range(min(AHEAD, nj * n)):
        for x in fetch(t // n, t % n, t):
            x.start()
    for t in tables:
        t.wait()
    for i, (m, which, row0, nr, _, _) in enumerate(jobs):
        col = jnp.transpose(tab_ref[which])[row0:row0 + nr, m:m + 1]
        r = lax.broadcasted_iota(jnp.int32, (nr, 2 * ne * cg), 1).astype(F32)
        sel_ref[:nr] = jnp.where(col == r, 1.0, 0.0).astype(BF16)

        def step(c, _):
            t = i * n + c
            for x in fetch(i, c, lax.rem(t, AHEAD + 1)):
                x.wait()

            def ahead(k, ck, tk):
                for x in fetch(k, ck, lax.rem(tk, AHEAD + 1)):
                    x.start()

            at(i, c + AHEAD, ahead)
            at(i, c - 2, lambda k, ck, tk: put(k, ck, lax.rem(tk, 2)).wait())
            rows = in_s[lax.rem(t, AHEAD + 1)]
            out_s[lax.rem(t, 2), :nr] = jnp.dot(sel_ref[:nr], rows, preferred_element_type=F32).astype(BF16)
            put(i, c, lax.rem(t, 2)).start()
            return 0

        lax.fori_loop(0, n, step, 0)
    for t in range(max(0, nj * n - 2), nj * n):
        put(t // n, t % n, t % 2).wait()


def pack(tok, o, sib, tabs, jobs, cg):
    _, ne, cap, d = o.shape
    arrays, full = [], []
    for job in jobs:
        a, ms = sib[job[0]]
        k = next((k for k, b in enumerate(arrays) if b is a), len(arrays))
        if k == len(arrays):
            arrays.append(a)
        full.append((*job, k, ms))
    n = d // CW
    most = max(job[3] for job in jobs)
    return pl.pallas_call(
        functools.partial(pack_kernel, full, ne, cg, cap // cg, n),
        in_specs=[ANY] * (4 + len(arrays)),
        out_specs=[ANY] * (len(jobs) + 1),
        out_shape=[jax.ShapeDtypeStruct((job[3], d), BF16) for job in jobs] + [TOK],
        input_output_aliases={0: len(jobs)},
        scratch_shapes=[pltpu.VMEM((AHEAD + 1, 2 * ne * cg, CW), BF16), pltpu.VMEM((2, most, CW), BF16),
                        pltpu.VMEM((most, 2 * ne * cg), BF16), pltpu.VMEM((2,) + tabs[0].shape, F32),
                        pltpu.SemaphoreType.DMA((AHEAD + 1, 2 * ne)), pltpu.SemaphoreType.DMA((2,)),
                        pltpu.SemaphoreType.DMA((2,))],
        compiler_params=pltpu.CompilerParams(vmem_limit_bytes=VMEM_LIMIT),
        cost_estimate=cost(2 * most * 2 * ne * cg * d * len(jobs)),
        name="pack",
    )(tok, o, *arrays, *tabs)


TB = 128
KW = 256


def combine_kernel(m, starts, tok, h, near, far, rest, tab, out, tok_out, h_s, near_s, far_s, out_s, sel_ref, gate_ref,
                   rank_ref, tab_ref, st_ref, isem, osem, tsem, rsem):
    nt, ncol = out_s.shape
    nb, full, fr = nt // TB, near_s.shape[0], far.shape[0]
    n = ncol // CW
    packed = (near_s, far_s)

    def fetch(c):
        ls = pl.ds(pl.multiple_of(c * CW, CW), CW)
        pairs = [(near.at[:, ls], near_s.at[:, ls]), (far.at[:, ls], far_s.at[pl.ds(0, fr), ls]),
                 (h.at[m, 0, :, ls], h_s.at[:, ls])]
        return [pltpu.make_async_copy(s, t, isem.at[c, e]) for e, (s, t) in enumerate(pairs)]

    def put(c):
        ls = pl.ds(pl.multiple_of(c * CW, CW), CW)
        return pltpu.make_async_copy(out_s.at[:, ls], out.at[:, ls], osem.at[c])

    def windows(b):
        ws, more = [], False
        for q in range(2):
            start, count = st_ref[((m * nb + b) * 2 + q) * 2], st_ref[((m * nb + b) * 2 + q) * 2 + 1]
            w = jnp.minimum(start - lax.rem(start, 16), full - KW)
            ws.append(pl.multiple_of(w, 16))
            more = jnp.logical_or(more, start + count > w + KW)
        return ws, more

    small = [pltpu.make_async_copy(tab.at[m], tab_ref, tsem.at[0]), pltpu.make_async_copy(starts, st_ref, tsem.at[1])]
    for x in small:
        x.start()
    for c in range(min(AHEAD, n)):
        for x in fetch(c):
            x.start()
    for x in small:
        x.wait()
    over = st_ref[st_ref.shape[0] - 1] > 0
    if fr < full:
        @pl.when(over)
        def _():
            x = pltpu.make_async_copy(rest, far_s.at[pl.ds(fr, full - fr)], rsem)
            x.start()
            x.wait()

        @pl.when(jnp.logical_not(over))
        def _():
            far_s[fr:, :] = jnp.zeros_like(far_s[fr:, :])

    cols = jnp.transpose(tab_ref[...])
    iw = lax.broadcasted_iota(jnp.int32, (TB, KW), 1).astype(F32)
    for k in range(2):
        gate_ref[k] = jnp.broadcast_to(cols[:, 4 + k:5 + k], (nt, 128))
        for q in range(2):
            rank_ref[k, q] = jnp.broadcast_to(cols[:, 2 * q + k:2 * q + k + 1], (nt, 128))
    for b in range(nb):
        ws, _ = windows(b)
        for k in range(2):
            for q in range(2):
                r = cols[b * TB:(b + 1) * TB, 2 * q + k:2 * q + k + 1] - ws[q].astype(F32)
                sel_ref[b, k * TB:(k + 1) * TB, q * KW:(q + 1) * KW] = jnp.where(r == iw, 1.0, 0.0).astype(BF16)

    def step(c, _):
        for x in fetch(c):
            x.wait()

        @pl.when(c + AHEAD < n)
        def _():
            for x in fetch(c + AHEAD):
                x.start()

        ls = pl.ds(pl.multiple_of(c * CW, CW), CW)

        def rows(ws):
            return jnp.concatenate([packed[q][pl.ds(ws[q], KW), ls] for q in range(2)], axis=0)

        for b in range(nb):
            ts = slice(b * TB, (b + 1) * TB)
            r = jnp.dot(sel_ref[b], rows(windows(b)[0]), preferred_element_type=F32)
            acc = h_s[ts, ls].astype(F32)
            for k in range(2):
                acc = acc + gate_ref[k, ts, :1] * r[k * TB:(k + 1) * TB]
            out_s[ts, ls] = acc.astype(BF16)

        def past(b, _):
            ws, more = windows(b)

            @pl.when(more)
            def _():
                ts = pl.ds(pl.multiple_of(b * TB, TB), TB)
                vs = [pl.multiple_of(jnp.minimum(w + KW, full - KW), 16) for w in ws]
                acc = h_s[ts, ls].astype(F32)
                for k in range(2):
                    sel = []
                    for q in range(2):
                        r = rank_ref[k, q, ts, :1]
                        r = jnp.where(r >= (ws[q] + KW).astype(F32), r - vs[q].astype(F32), -1.0)
                        sel.append(jnp.where(r == iw, 1.0, 0.0).astype(BF16))
                    r = jnp.dot(jnp.concatenate(sel, axis=1), rows(vs), preferred_element_type=F32)
                    r += jnp.dot(sel_ref[b, k * TB:(k + 1) * TB], rows(ws), preferred_element_type=F32)
                    acc = acc + gate_ref[k, ts, :1] * r
                out_s[ts, ls] = acc.astype(BF16)

            return 0

        lax.fori_loop(0, nb, past, 0)
        put(c).start()
        return 0

    lax.fori_loop(0, n, step, 0)
    for c in range(n):
        put(c).wait()


def combine(starts, tok, h, near, far, rest, tab, m):
    nt, d = h.shape[2:]
    full = near.shape[0]
    n = d // CW
    return pl.pallas_call(
        functools.partial(combine_kernel, m),
        in_specs=[ANY] * 7,
        out_specs=[ANY, ANY],
        out_shape=[jax.ShapeDtypeStruct((nt, d), BF16), TOK],
        input_output_aliases={1: 1},
        scratch_shapes=[pltpu.VMEM((nt, d), BF16), pltpu.VMEM((full, d), BF16), pltpu.VMEM((full, d), BF16),
                        pltpu.VMEM((nt, d), BF16), pltpu.VMEM((nt // TB, 2 * TB, 2 * KW), BF16),
                        pltpu.VMEM((2, nt, 128), F32), pltpu.VMEM((2, 2, nt, 128), F32),
                        pltpu.VMEM(tab.shape[1:], F32), pltpu.SMEM(starts.shape, jnp.int32),
                        pltpu.SemaphoreType.DMA((n, 3)), pltpu.SemaphoreType.DMA((n,)), pltpu.SemaphoreType.DMA((2,)),
                        pltpu.SemaphoreType.DMA],
        compiler_params=pltpu.CompilerParams(vmem_limit_bytes=VMEM_LIMIT),
        cost_estimate=cost(4 * nt * 2 * KW * d),
        name="combine",
    )(starts, tok, h, near, far, rest, tab)


def nothing_kernel(tok, *refs):
    pass


def nothing(tok, shapes):
    return pl.pallas_call(nothing_kernel, in_specs=[ANY], out_specs=[ANY] * (len(shapes) + 1),
                          out_shape=[jax.ShapeDtypeStruct(s, BF16) for s in shapes] + [TOK],
                          input_output_aliases={0: len(shapes)}, name="nothing")(tok)


G = 4
QB = 256
NR = 6


def scores(q, k, h, p_s, l_s):
    nt = q.shape[0]
    sc = (HD ** -0.5) * math.log2(math.e)
    off = 0
    for q0 in range(0, nt, QB):
        kn = q0 + QB
        s = lax.dot_general(q[q0:kn], k[:kn], (((1,), (1,)), ((), ())), preferred_element_type=F32)
        r = lax.broadcasted_iota(jnp.int32, (QB, QB), 0)
        c = lax.broadcasted_iota(jnp.int32, (QB, QB), 1)
        sd = jnp.where(r >= c, s[:, q0:], -1e30)
        s = sd if q0 == 0 else jnp.concatenate([s[:, :q0], sd], axis=1)
        mx = jnp.max(s, axis=1, keepdims=True)
        p = jnp.exp2(s * sc - mx * sc)
        p_s[h, :, off:off + kn] = p
        l_s[h, q0:kn, :] = jnp.broadcast_to(jnp.sum(p, axis=1, keepdims=True), (QB, HD))
        off += kn


def layer_kernel(first, npiece, *refs):
    us, refs = refs[:npiece], refs[npiece:]
    if not first:
        refs = refs[1:]
    (m_ref, _, w_ref, wq, wk, wv, wo, z_hbm, _, u_s, x_s, a_s, q_s, k_s, v_s, z_s, p_s, l_s, ring, rsem, usem,
     zsem) = refs
    nt, d = u_s.shape
    m = m_ref[0]
    gc = G * HD
    ng = d // gc
    uc = 4
    if npiece == 1:
        cr = nt // uc
        ucp = [pltpu.make_async_copy(us[0].at[pl.ds(c * cr, cr)], u_s.at[pl.ds(c * cr, cr)], usem.at[c])
               for c in range(uc)]
    else:
        cw = d // npiece
        ucp = [pltpu.make_async_copy(us[c], u_s.at[:, pl.ds(c * cw, cw)], usem.at[c]) for c in range(npiece)]
    for c in ucp:
        c.start()

    def wcopy(ref, col, slot):
        return pltpu.make_async_copy(ref.at[:, pl.ds(pl.multiple_of(col * gc, gc), gc)], ring.at[slot], rsem.at[slot])

    def qkv_start(i):
        b = lax.rem(i, 2) * 3
        for c, r in enumerate((wq, wk, wv)):
            wcopy(r, i, b + c).start()

    def wo_start(j):
        wcopy(wo, j, lax.rem(3 * ng + j, NR)).start()

    def wait(slot):
        wcopy(wq, 0, slot).wait()

    qkv_start(0)
    ch = 64

    def norm(r0, n):
        def f(t, _):
            rs = pl.ds(pl.multiple_of(r0 + t * ch, ch), ch)
            uf = u_s[rs, :].astype(F32)
            x_s[rs, :] = (uf * lax.rsqrt(jnp.mean(uf * uf, axis=-1, keepdims=True) + EPS) * w_ref[...]).astype(BF16)
            return 0

        lax.fori_loop(0, n // ch, f, 0)

    for c in range(len(ucp)):
        ucp[c].wait()
        if npiece == 1:
            norm(c * cr, cr)
    if npiece > 1:
        norm(0, nt)

    def attend(i):
        for h in range(G):
            off = 0
            for q0 in range(0, nt, QB):
                kn = q0 + QB
                p = p_s[h, :, off:off + kn]
                off += kn
                v = v_s[:kn, h * HD:(h + 1) * HD].astype(F32)
                o = jnp.dot(p, v, preferred_element_type=F32) / l_s[h, q0:kn, :]
                a_s[q0:kn, pl.ds(pl.multiple_of(i * gc, gc) + h * HD, HD)] = o.astype(BF16)

    def group(i, _):
        b = lax.rem(i, 2) * 3
        for c in range(3):
            wait(b + c)

        @pl.when(i + 1 < ng)
        def _():
            qkv_start(i + 1)

        @pl.when(i + 1 >= ng)
        def _():
            for j in range(3):
                wo_start(j)

        attend(jnp.maximum(i - 1, 0))
        q_s[...] = jnp.dot(x_s[...], ring[b], preferred_element_type=F32).astype(BF16)
        k_s[...] = jnp.dot(x_s[...], ring[b + 1], preferred_element_type=F32).astype(BF16)
        for h in range(G):
            scores(q_s[:, h * HD:(h + 1) * HD], k_s[:, h * HD:(h + 1) * HD], h, p_s, l_s)
        v_s[...] = jnp.dot(x_s[...], ring[b + 2], preferred_element_type=F32).astype(BF16)
        return 0

    lax.fori_loop(0, ng, group, 0)
    wo_start(3)
    attend(ng - 1)

    def zcopy(j):
        cs = pl.ds(pl.multiple_of(j * gc, gc), gc)
        return pltpu.make_async_copy(z_s.at[:, cs], z_hbm.at[m, 0, :, cs], zsem.at[j])

    def wo_step(jj, _):
        for e in range(2):
            wait(lax.rem(3 * ng + jj * 2 + e, NR))
        for e in range(2):
            @pl.when(jj * 2 + e + 4 < ng)
            def _():
                wo_start(jj * 2 + e + 4)
        for e in range(2):
            j = jj * 2 + e
            y = jnp.dot(a_s[...], ring[lax.rem(3 * ng + j, NR)], preferred_element_type=F32).astype(BF16).astype(F32)
            cs = pl.ds(pl.multiple_of(j * gc, gc), gc)
            z_s[:, cs] = (u_s[:, cs].astype(F32) + y).astype(BF16)
        for e in range(2):
            zcopy(jj * 2 + e).start()
        return 0

    lax.fori_loop(0, ng // 2, wo_step, 0)
    for j in range(ng):
        zcopy(j).wait()


def layer(us, z, m, tok, w, wq, wk, wv, wo, mb):
    nt, d = us[0].shape[0], wq.shape[0]
    first = z is None
    n = len(us)
    ng = d // (G * HD)
    smem = pl.BlockSpec(memory_space=pltpu.SMEM)
    vmem = pl.BlockSpec(memory_space=pltpu.VMEM)
    ins = list(us) + ([] if first else [z]) + [jnp.full((1,), m, jnp.int32), tok, w, wq, wk, wv, wo]
    specs = [ANY] * n + ([] if first else [ANY]) + [smem, ANY, vmem] + [ANY] * 4
    alias = {} if first else {n: 0}
    alias[len(specs) - 6] = 1
    pw = sum(range(QB, nt + 1, QB))
    return pl.pallas_call(
        functools.partial(layer_kernel, first, n),
        in_specs=specs,
        out_specs=[ANY, ANY],
        out_shape=[jax.ShapeDtypeStruct((mb, 1, nt, d), BF16), TOK],
        input_output_aliases=alias,
        scratch_shapes=[pltpu.VMEM((nt, d), BF16)] * 3 + [pltpu.VMEM((nt, G * HD), BF16)] * 3 + [
            pltpu.VMEM((nt, d), BF16), pltpu.VMEM((G, QB, pw), F32), pltpu.VMEM((G, nt, HD), F32),
            pltpu.VMEM((NR, d, G * HD), BF16), pltpu.SemaphoreType.DMA((NR,)),
            pltpu.SemaphoreType.DMA((max(4, n),)), pltpu.SemaphoreType.DMA((ng,))],
        compiler_params=pltpu.CompilerParams(vmem_limit_bytes=VMEM_LIMIT),
        cost_estimate=cost(8 * nt * d * d + 4 * nt * nt * d),
        name="layer",
    )(*ins)


def tables(idx, slot, gate, x, c, j, ne, cg):
    mb, nt, top = idx.shape
    valid = slot >= 0
    core = (idx // ne) % 2
    row = jnp.where(core == c, 0, ne * cg) + (idx % ne) * cg + slot - j * cg
    row = row.reshape(mb, 1, nt * top)
    other = idx // (2 * ne) != x
    place = jnp.arange(2 * ne * cg, dtype=jnp.int32)[None, :, None]
    ranks, starts, rows, counts = [], [], [], []
    for mine in (valid & ~other, valid & other):
        flat = mine.reshape(mb, nt * top)
        rank = jnp.cumsum(flat.astype(jnp.int32), axis=1) - 1
        at = jnp.where(flat, rank, -1)
        ranks.append(at.reshape(mb, nt, top).astype(F32))
        count = flat.reshape(mb, nt // TB, TB * top).sum(-1, dtype=jnp.int32)
        starts.append(jnp.stack([jnp.cumsum(count, axis=1) - count, count], axis=-1))
        rows.append((jnp.sum(jnp.where(at[:, None, :] == place, row + 1, 0), axis=-1) - 1).astype(F32))
        counts.append(count.sum(-1))
    cols = jnp.stack([v[..., k] for v in (*ranks, gate) for k in range(top)], axis=1)
    return cols, jnp.stack(starts, axis=2), rows, jnp.maximum(*counts)


CAP = 576


def order(mb):
    r = [('r', k, k) for k in range(3)]
    c = [('c', m, m) for m in range(mb)]
    half = (mb + 2) // 2
    out = [('p', 0, 1), ('s', 1, 2)] + r[:1] + [('b', 0, 2), ('e', 0, 2), ('s', 2, mb)] + r[1:2] + c[:1] + r[2:]
    out += [('b', 2, half), ('b', half, mb), ('e', 2, mb)] + c[1:2]
    for m in range(mb):
        out += [('l', m, m)]
        if m + 2 < mb:
            out += c[m + 2:m + 3]
    return out


def solution(mesh):
    npp, nep = mesh.shape['pp'], mesh.shape['ep']
    over = [(i, (i + 1) % npp) for i in range(npp)]
    peer = [(i, (i + nep // 2) % nep) for i in range(nep)]
    sibling = [(i, i ^ 1) for i in range(nep)]
    tok_spec = P(('data', 'pp'), None, 'ep', None, None)
    wsp = P('pp', None, None, None)

    def body(O, idx, slot, g, H, w, Wq, Wk, Wv, Wo):
        o, h = O[0], H[0]
        mb, ne, cap, d = o.shape
        cg = cap // nep
        nt = h.shape[2]
        j = lax.axis_index('ep')
        x, c = j // 2, j % 2
        three = lambda a: a[0].reshape(mb, nt, a.shape[-1])
        cols, starts, rows, need = tables(three(idx), three(slot), three(g), x, c, j, ne, cg)
        send = jnp.stack([2 * x + 1 - c, (2 * x + 1 - c + 2) % nep]).astype(jnp.int32)
        fresh = jnp.zeros((8, 128), F32)
        wqkv = [a[0] for a in (Wq, Wk, Wv)]
        wo = Wo[0].reshape(d, d)

        full = 2 * ne * cg
        s0, tok = slice_rows(send, fresh, o, 0, 1, cg)
        d0 = lax.ppermute(s0, 'ep', sibling)
        tabs = [rows[NEAR], lax.ppermute(rows[FAR], 'ep', peer)]

        def run(tok, sib):
            over_cap = (need > CAP).astype(jnp.int32).max().reshape(1)
            for axis, pairs in (('ep', peer), ('pp', over), ('ep', sibling)):
                over_cap = jnp.maximum(over_cap, lax.ppermute(over_cap, axis, pairs))
            st = jnp.concatenate([starts.reshape(-1), jnp.broadcast_to(over_cap, (128,))])
            near, far, packed, rest, ys = {}, {}, {}, {}, {}
            z = None
            for kind, m, e in order(mb):
                if kind == 's':
                    s, tok = slice_rows(send, tok, o, m, e - m, cg)
                    s = lax.ppermute(s, 'ep', sibling)
                    for i in range(m, e):
                        sib[i] = (s, i - m)
                elif kind == 'r':
                    v, tok = lax.optimization_barrier((wqkv[m], tok))
                    wqkv[m], tok = lax.optimization_barrier((jnp.reshape(v, (d, d)), tok))
                elif kind in 'pb':
                    jobs = [(i, w_, 0, CAP if w_ == FAR else full) for i in range(m, e) for w_ in (FAR, NEAR)]
                    jobs = [b for b in jobs if (b[1] == FAR) == (kind == 'p') or b[0] > 0]
                    *out, tok = pack(tok, o, sib, tabs, jobs, cg)
                    for b, r in zip(jobs, out):
                        if b[1] == NEAR:
                            near[b[0]] = r
                        elif b[0] == 0:
                            far[0] = lax.ppermute(r, 'ep', peer)
                        else:
                            packed[b[0]] = r
                elif kind == 'e':
                    def past(tok):
                        *out, tok = pack(tok, o, sib, tabs, [(i, FAR, CAP, full - CAP) for i in range(m, e)], cg)
                        return [lax.ppermute(v, 'ep', peer) for v in out] + [tok]

                    def none(tok):
                        return list(nothing(tok, [(full - CAP, d)] * (e - m)))

                    *out, tok = lax.cond(over_cap[0] > 0, past, none, tok)
                    rest.update(zip(range(m, e), out))
                    for i in sorted(packed):
                        v, tok = lax.optimization_barrier((packed.pop(i), tok))
                        far[i] = lax.ppermute(v, 'ep', peer)
                elif kind == 'c':
                    y, tok = combine(st, tok, h, near[m], far[m], rest[m], cols, m)
                    ys[m] = [lax.ppermute(y, 'pp', over)]
                else:
                    z, tok = layer(ys[m], z, m, tok, w, *wqkv, wo, mb)
            return z

        return run(tok, {0: (d0, 0)})[None]

    return jax.shard_map(body, mesh=mesh,
                         in_specs=(tok_spec, tok_spec, tok_spec, tok_spec, tok_spec, P('pp', None), wsp, wsp, wsp, wsp),
                         out_specs=tok_spec, check_vma=False)
```

```python
import functools
import math

import jax
import jax.numpy as jnp
from jax import lax
from jax.experimental import pallas as pl
from jax.experimental.pallas import tpu as pltpu
from jax.sharding import PartitionSpec as P


EPS = 1e-6
HD = 128
F32 = jnp.float32
BF16 = jnp.bfloat16
VMEM_LIMIT = 63 * 1024 * 1024
ANY = pl.BlockSpec(memory_space=pltpu.HBM)
TOK = jax.ShapeDtypeStruct((8, 128), F32)


def cost(flops):
    return pl.CostEstimate(flops=int(flops), bytes_accessed=int(flops) // 256, transcendentals=0)


def slice_kernel(rows_ref, tok, o_ref, out_ref, tok_out):
    out_ref[...] = o_ref[...].reshape(out_ref.shape)


def slice_rows(rows, tok, o, m0, nm, cg):
    _, ne, _, d = o.shape
    n_own = rows.shape[0]
    return pl.pallas_call(
        slice_kernel,
        grid_spec=pltpu.PrefetchScalarGridSpec(
            num_scalar_prefetch=1,
            grid=(nm, n_own),
            in_specs=[ANY, pl.BlockSpec((1, ne, cg, d), lambda m, a, r: (m0 + m, 0, r[a], 0))],
            out_specs=[pl.BlockSpec((1, 1, ne, cg, d), lambda m, a, r: (m, a, 0, 0, 0)), ANY],
        ),
        out_shape=[jax.ShapeDtypeStruct((nm, n_own, ne, cg, d), o.dtype), TOK],
        input_output_aliases={1: 1},
        compiler_params=pltpu.CompilerParams(vmem_limit_bytes=VMEM_LIMIT),
        cost_estimate=cost(nm * 2e9),
        name="slice_rows",
    )(rows, tok, o)


PW = 2048
CW = 1024
AHEAD = 2
FAR, NEAR = 1, 0


def pack_kernel(jobs, ne, cg, nep, n, *refs):
    nj = len(jobs)
    nsib = 1 + max(job[4] for job in jobs)
    o = refs[1]
    sibs, tabs = refs[2:2 + nsib], refs[2 + nsib:4 + nsib]
    outs = refs[4 + nsib:4 + nsib + nj]
    _, in_s, out_s, sel_ref, tab_ref, isem, osem, tsem = refs[4 + nsib + nj:]
    j = lax.axis_index('ep')
    firsts = (j * cg, lax.rem(j + nep // 2, nep) * cg)

    def fetch(i, c, slot):
        m, which, _, _, s, ms = jobs[i]
        cs = pl.ds(pl.multiple_of(c * PW, PW), PW)
        rs = pl.ds(pl.multiple_of(firsts[which], 16), cg)
        src = [o.at[m, e, rs, cs] for e in range(ne)]
        src += [sibs[s].at[ms, which, e, :, cs] for e in range(ne)]
        return [pltpu.make_async_copy(v, in_s.at[slot, pl.ds(e * cg, cg)], isem.at[slot, e]) for e, v in enumerate(src)]

    def put(i, c, slot):
        ls = pl.ds(pl.multiple_of(c * PW, PW), PW)
        return pltpu.make_async_copy(out_s.at[slot, pl.ds(0, jobs[i][3])], outs[i].at[:, ls], osem.at[slot])

    def at(i, c, f):
        for k, lo in ((i - 1, -n), (i, 0), (i + 1, n)):
            if 0 <= k < nj:
                @pl.when(jnp.logical_and(c >= lo, c < lo + n))
                def _():
                    f(k, c - lo, i * n + c)

    tables = [pltpu.make_async_copy(t, tab_ref.at[k], tsem.at[k]) for k, t in enumerate(tabs)]
    for t in tables:
        t.start()
    for t in range(min(AHEAD, nj * n)):
        for x in fetch(t // n, t % n, t):
            x.start()
    for t in tables:
        t.wait()
    for i, (m, which, row0, nr, _, _) in enumerate(jobs):
        col = jnp.transpose(tab_ref[which])[row0:row0 + nr, m:m + 1]
        r = lax.broadcasted_iota(jnp.int32, (nr, 2 * ne * cg), 1).astype(F32)
        sel_ref[:nr] = jnp.where(col == r, 1.0, 0.0).astype(BF16)

        def step(c, _):
            t = i * n + c
            for x in fetch(i, c, lax.rem(t, AHEAD + 1)):
                x.wait()

            def ahead(k, ck, tk):
                for x in fetch(k, ck, lax.rem(tk, AHEAD + 1)):
                    x.start()

            at(i, c + AHEAD, ahead)
            at(i, c - 2, lambda k, ck, tk: put(k, ck, lax.rem(tk, 2)).wait())
            rows = in_s[lax.rem(t, AHEAD + 1)]
            out_s[lax.rem(t, 2), :nr] = jnp.dot(sel_ref[:nr], rows, preferred_element_type=F32).astype(BF16)
            put(i, c, lax.rem(t, 2)).start()
            return 0

        lax.fori_loop(0, n, step, 0)
    for t in range(max(0, nj * n - 2), nj * n):
        put(t // n, t % n, t % 2).wait()


def pack(tok, o, sib, tabs, jobs, cg):
    _, ne, cap, d = o.shape
    arrays, full = [], []
    for job in jobs:
        a, ms = sib[job[0]]
        k = next((k for k, b in enumerate(arrays) if b is a), len(arrays))
        if k == len(arrays):
            arrays.append(a)
        full.append((*job, k, ms))
    n = d // PW
    most = max(job[3] for job in jobs)
    return pl.pallas_call(
        functools.partial(pack_kernel, full, ne, cg, cap // cg, n),
        in_specs=[ANY] * (4 + len(arrays)),
        out_specs=[ANY] * (len(jobs) + 1),
        out_shape=[jax.ShapeDtypeStruct((job[3], d), BF16) for job in jobs] + [TOK],
        input_output_aliases={0: len(jobs)},
        scratch_shapes=[pltpu.VMEM((AHEAD + 1, 2 * ne * cg, PW), BF16), pltpu.VMEM((2, most, PW), BF16),
                        pltpu.VMEM((most, 2 * ne * cg), BF16), pltpu.VMEM((2,) + tabs[0].shape, F32),
                        pltpu.SemaphoreType.DMA((AHEAD + 1, 2 * ne)), pltpu.SemaphoreType.DMA((2,)),
                        pltpu.SemaphoreType.DMA((2,))],
        compiler_params=pltpu.CompilerParams(vmem_limit_bytes=VMEM_LIMIT),
        cost_estimate=cost(2 * most * 2 * ne * cg * d * len(jobs)),
        name="pack",
    )(tok, o, *arrays, *tabs)


TB = 128
KW = 256
NST = 128
CAHEAD = 2


def combine_kernel(m, full, starts, tok, h, near, far, near_rest, far_rest, tab, out, tok_out, h_s, near_s, far_s, out_s, sel_ref, gate_ref,
                   rank_ref, tab_ref, st_ref, isem, osem, tsem, rsem):
    nt, ncol = out_s.shape
    nb, cap = nt // TB, near.shape[0]
    n = ncol // CW
    packed = (near_s, far_s)

    def fetch(c):
        ls = pl.ds(pl.multiple_of(c * CW, CW), CW)
        pairs = [(near.at[:, ls], near_s.at[pl.ds(0, cap), ls]), (far.at[:, ls], far_s.at[pl.ds(0, cap), ls]),
                 (h.at[m, 0, :, ls], h_s.at[:, ls])]
        return [pltpu.make_async_copy(s, t, isem.at[c, e]) for e, (s, t) in enumerate(pairs)]

    def put(c):
        ls = pl.ds(pl.multiple_of(c * CW, CW), CW)
        return pltpu.make_async_copy(out_s.at[:, ls], out.at[:, ls], osem.at[c])

    def windows(b):
        ws, more = [], False
        for q in range(2):
            start, count = st_ref[(b * 2 + q) * 2], st_ref[(b * 2 + q) * 2 + 1]
            w = jnp.minimum(start - lax.rem(start, 16), full - KW)
            ws.append(pl.multiple_of(w, 16))
            more = jnp.logical_or(more, start + count > w + KW)
        return ws, more

    small = [pltpu.make_async_copy(tab.at[m], tab_ref, tsem.at[0]), pltpu.make_async_copy(starts.at[pl.ds(m * 128, NST)], st_ref, tsem.at[1])]
    for x in small:
        x.start()
    for c in range(min(CAHEAD, n)):
        for x in fetch(c):
            x.start()
    for x in small:
        x.wait()
    over = st_ref[nb * 4] > 0
    if cap < full:
        @pl.when(over)
        def _():
            past = [pltpu.make_async_copy(r, p.at[pl.ds(cap, full - cap)], rsem.at[q])
                    for q, (r, p) in enumerate(zip((near_rest, far_rest), packed))]
            for x in past:
                x.start()
            for x in past:
                x.wait()

        @pl.when(jnp.logical_not(over))
        def _():
            for p in packed:
                p[cap:, :] = jnp.zeros_like(p[cap:, :])

    cols = jnp.transpose(tab_ref[...])
    iw = lax.broadcasted_iota(jnp.int32, (TB, KW), 1).astype(F32)
    for k in range(2):
        gate_ref[k] = jnp.broadcast_to(cols[:, 4 + k:5 + k], (nt, 128))
        for q in range(2):
            rank_ref[k, q] = jnp.broadcast_to(cols[:, 2 * q + k:2 * q + k + 1], (nt, 128))
    for b in range(nb):
        ws, _ = windows(b)
        for k in range(2):
            for q in range(2):
                r = cols[b * TB:(b + 1) * TB, 2 * q + k:2 * q + k + 1] - ws[q].astype(F32)
                sel_ref[b, k * TB:(k + 1) * TB, q * KW:(q + 1) * KW] = jnp.where(r == iw, 1.0, 0.0).astype(BF16)

    def step(c, _):
        for x in fetch(c):
            x.wait()

        @pl.when(c + CAHEAD < n)
        def _():
            for x in fetch(c + CAHEAD):
                x.start()

        ls = pl.ds(pl.multiple_of(c * CW, CW), CW)

        def rows(ws):
            return jnp.concatenate([packed[q][pl.ds(ws[q], KW), ls] for q in range(2)], axis=0)

        for b in range(nb):
            ts = slice(b * TB, (b + 1) * TB)
            r = jnp.dot(sel_ref[b], rows(windows(b)[0]), preferred_element_type=F32)
            acc = h_s[ts, ls].astype(F32)
            for k in range(2):
                acc = acc + gate_ref[k, ts, :1] * r[k * TB:(k + 1) * TB]
            out_s[ts, ls] = acc.astype(BF16)

        def past(b, _):
            ws, more = windows(b)

            @pl.when(more)
            def _():
                ts = pl.ds(pl.multiple_of(b * TB, TB), TB)
                vs = [pl.multiple_of(jnp.minimum(w + KW, full - KW), 16) for w in ws]
                acc = h_s[ts, ls].astype(F32)
                for k in range(2):
                    sel = []
                    for q in range(2):
                        r = rank_ref[k, q, ts, :1]
                        r = jnp.where(r >= (ws[q] + KW).astype(F32), r - vs[q].astype(F32), -1.0)
                        sel.append(jnp.where(r == iw, 1.0, 0.0).astype(BF16))
                    r = jnp.dot(jnp.concatenate(sel, axis=1), rows(vs), preferred_element_type=F32)
                    r += jnp.dot(sel_ref[b, k * TB:(k + 1) * TB], rows(ws), preferred_element_type=F32)
                    acc = acc + gate_ref[k, ts, :1] * r
                out_s[ts, ls] = acc.astype(BF16)

            return 0

        lax.fori_loop(0, nb, past, 0)
        put(c).start()
        return 0

    lax.fori_loop(0, n, step, 0)
    for c in range(n):
        put(c).wait()


def combine(starts, tok, h, near, far, near_rest, far_rest, tab, m, full):
    nt, d = h.shape[2:]
    n = d // CW
    return pl.pallas_call(
        functools.partial(combine_kernel, m, full),
        in_specs=[ANY] * 8,
        out_specs=[ANY, ANY],
        out_shape=[jax.ShapeDtypeStruct((nt, d), BF16), TOK],
        input_output_aliases={1: 1},
        scratch_shapes=[pltpu.VMEM((nt, d), BF16), pltpu.VMEM((full, d), BF16), pltpu.VMEM((full, d), BF16),
                        pltpu.VMEM((nt, d), BF16), pltpu.VMEM((nt // TB, 2 * TB, 2 * KW), BF16),
                        pltpu.VMEM((2, nt, 128), F32), pltpu.VMEM((2, 2, nt, 128), F32),
                        pltpu.VMEM(tab.shape[1:], F32), pltpu.SMEM((NST,), jnp.int32),
                        pltpu.SemaphoreType.DMA((n, 3)), pltpu.SemaphoreType.DMA((n,)), pltpu.SemaphoreType.DMA((2,)),
                        pltpu.SemaphoreType.DMA((2,))],
        compiler_params=pltpu.CompilerParams(vmem_limit_bytes=VMEM_LIMIT),
        cost_estimate=cost(4 * nt * 2 * KW * d),
        name="combine",
    )(starts, tok, h, near, far, near_rest, far_rest, tab)


def nothing_kernel(tok, *refs):
    pass


def nothing(tok, shapes):
    return pl.pallas_call(nothing_kernel, in_specs=[ANY], out_specs=[ANY] * (len(shapes) + 1),
                          out_shape=[jax.ShapeDtypeStruct(s, BF16) for s in shapes] + [TOK],
                          input_output_aliases={0: len(shapes)}, name="nothing")(tok)


G = 4
QB = 256
NR = 6


def scores(q, k, h, p_s, l_s):
    nt = q.shape[0]
    sc = (HD ** -0.5) * math.log2(math.e)
    off = 0
    for q0 in range(0, nt, QB):
        kn = q0 + QB
        s = lax.dot_general(q[q0:kn], k[:kn], (((1,), (1,)), ((), ())), preferred_element_type=F32)
        r = lax.broadcasted_iota(jnp.int32, (QB, QB), 0)
        c = lax.broadcasted_iota(jnp.int32, (QB, QB), 1)
        sd = jnp.where(r >= c, s[:, q0:], -1e30)
        s = sd if q0 == 0 else jnp.concatenate([s[:, :q0], sd], axis=1)
        mx = jnp.max(s, axis=1, keepdims=True)
        p = jnp.exp2(s * sc - mx * sc)
        p_s[h, :, off:off + kn] = p
        l_s[h, q0:kn, :] = jnp.broadcast_to(jnp.sum(p, axis=1, keepdims=True), (QB, HD))
        off += kn


def layer_kernel(m, first, npiece, *refs):
    us, refs = refs[:npiece], refs[npiece:]
    if not first:
        refs = refs[1:]
    (_, w, wq, wk, wv, wo, z_hbm, _, u_s, x_s, a_s, q_s, k_s, v_s, z_s, p_s, l_s, ring, w_ref, rsem, usem, zsem,
     wsem) = refs
    nt, d = u_s.shape
    gc = G * HD
    ng = d // gc
    uc = 4
    if npiece == 1:
        cr = nt // uc
        ucp = [pltpu.make_async_copy(us[0].at[pl.ds(c * cr, cr)], u_s.at[pl.ds(c * cr, cr)], usem.at[c])
               for c in range(uc)]
    else:
        cw = d // npiece
        ucp = [pltpu.make_async_copy(us[c], u_s.at[:, pl.ds(c * cw, cw)], usem.at[c]) for c in range(npiece)]
    gain = pltpu.make_async_copy(w, w_ref, wsem)
    gain.start()
    for c in ucp:
        c.start()

    def wcopy(ref, col, slot):
        return pltpu.make_async_copy(ref.at[:, pl.ds(pl.multiple_of(col * gc, gc), gc)], ring.at[slot], rsem.at[slot])

    def qkv_start(i):
        b = lax.rem(i, 2) * 3
        for c, r in enumerate((wq, wk, wv)):
            wcopy(r, i, b + c).start()

    def wo_start(j):
        wcopy(wo, j, lax.rem(3 * ng + j, NR)).start()

    def wait(slot):
        wcopy(wq, 0, slot).wait()

    qkv_start(0)
    ch = 64

    def norm(r0, n):
        def f(t, _):
            rs = pl.ds(pl.multiple_of(r0 + t * ch, ch), ch)
            uf = u_s[rs, :].astype(F32)
            x_s[rs, :] = (uf * lax.rsqrt(jnp.mean(uf * uf, axis=-1, keepdims=True) + EPS) * w_ref[...]).astype(BF16)
            return 0

        lax.fori_loop(0, n // ch, f, 0)

    gain.wait()
    for c in range(len(ucp)):
        ucp[c].wait()
        if npiece == 1:
            norm(c * cr, cr)
    if npiece > 1:
        norm(0, nt)

    def attend(i):
        for h in range(G):
            off = 0
            for q0 in range(0, nt, QB):
                kn = q0 + QB
                p = p_s[h, :, off:off + kn]
                off += kn
                v = v_s[:kn, h * HD:(h + 1) * HD].astype(F32)
                o = jnp.dot(p, v, preferred_element_type=F32) / l_s[h, q0:kn, :]
                a_s[q0:kn, pl.ds(pl.multiple_of(i * gc, gc) + h * HD, HD)] = o.astype(BF16)

    def group(i, _):
        b = lax.rem(i, 2) * 3
        for c in range(3):
            wait(b + c)

        @pl.when(i + 1 < ng)
        def _():
            qkv_start(i + 1)

        @pl.when(i + 1 >= ng)
        def _():
            for j in range(3):
                wo_start(j)

        attend(jnp.maximum(i - 1, 0))
        q_s[...] = jnp.dot(x_s[...], ring[b], preferred_element_type=F32).astype(BF16)
        k_s[...] = jnp.dot(x_s[...], ring[b + 1], preferred_element_type=F32).astype(BF16)
        for h in range(G):
            scores(q_s[:, h * HD:(h + 1) * HD], k_s[:, h * HD:(h + 1) * HD], h, p_s, l_s)
        v_s[...] = jnp.dot(x_s[...], ring[b + 2], preferred_element_type=F32).astype(BF16)
        return 0

    lax.fori_loop(0, ng, group, 0)
    wo_start(3)
    attend(ng - 1)

    def zcopy(j):
        cs = pl.ds(pl.multiple_of(j * gc, gc), gc)
        return pltpu.make_async_copy(z_s.at[:, cs], z_hbm.at[m, 0, :, cs], zsem.at[j])

    def wo_step(jj, _):
        for e in range(2):
            wait(lax.rem(3 * ng + jj * 2 + e, NR))
        for e in range(2):
            @pl.when(jj * 2 + e + 4 < ng)
            def _():
                wo_start(jj * 2 + e + 4)
        for e in range(2):
            j = jj * 2 + e
            y = jnp.dot(a_s[...], ring[lax.rem(3 * ng + j, NR)], preferred_element_type=F32).astype(BF16).astype(F32)
            cs = pl.ds(pl.multiple_of(j * gc, gc), gc)
            z_s[:, cs] = (u_s[:, cs].astype(F32) + y).astype(BF16)
        for e in range(2):
            zcopy(jj * 2 + e).start()
        return 0

    lax.fori_loop(0, ng // 2, wo_step, 0)
    for j in range(ng):
        zcopy(j).wait()


def layer(us, z, m, tok, w, wq, wk, wv, wo, mb):
    nt, d = us[0].shape[0], wq.shape[0]
    first = z is None
    n = len(us)
    ng = d // (G * HD)
    ins = list(us) + ([] if first else [z]) + [tok, w, wq, wk, wv, wo]
    alias = {} if first else {n: 0}
    alias[len(ins) - 6] = 1
    pw = sum(range(QB, nt + 1, QB))
    return pl.pallas_call(
        functools.partial(layer_kernel, m, first, n),
        in_specs=[ANY] * len(ins),
        out_specs=[ANY, ANY],
        out_shape=[jax.ShapeDtypeStruct((mb, 1, nt, d), BF16), TOK],
        input_output_aliases=alias,
        scratch_shapes=[pltpu.VMEM((nt, d), BF16)] * 3 + [pltpu.VMEM((nt, G * HD), BF16)] * 3 + [
            pltpu.VMEM((nt, d), BF16), pltpu.VMEM((G, QB, pw), F32), pltpu.VMEM((G, nt, HD), F32),
            pltpu.VMEM((NR, d, G * HD), BF16), pltpu.VMEM((1, d), F32), pltpu.SemaphoreType.DMA((NR,)),
            pltpu.SemaphoreType.DMA((max(4, n),)), pltpu.SemaphoreType.DMA((ng,)), pltpu.SemaphoreType.DMA],
        compiler_params=pltpu.CompilerParams(vmem_limit_bytes=VMEM_LIMIT),
        cost_estimate=cost(8 * nt * d * d + 4 * nt * nt * d),
        name="layer",
    )(*ins)


def tables(idx, slot, gate, x, c, j, ne, cg):
    mb, nt, top = idx.shape
    valid = slot >= 0
    core = (idx // ne) % 2
    row = jnp.where(core == c, 0, ne * cg) + (idx % ne) * cg + slot - j * cg
    row = row.reshape(mb, 1, nt * top)
    other = idx // (2 * ne) != x
    place = jnp.arange(2 * ne * cg, dtype=jnp.int32)[None, :, None]
    ranks, starts, rows, counts = [], [], [], []
    for mine in (valid & ~other, valid & other):
        flat = mine.reshape(mb, nt * top)
        rank = jnp.cumsum(flat.astype(jnp.int32), axis=1) - 1
        at = jnp.where(flat, rank, -1)
        ranks.append(at.reshape(mb, nt, top).astype(F32))
        count = flat.reshape(mb, nt // TB, TB * top).sum(-1, dtype=jnp.int32)
        starts.append(jnp.stack([jnp.cumsum(count, axis=1) - count, count], axis=-1))
        rows.append((jnp.sum(jnp.where(at[:, None, :] == place, row + 1, 0), axis=-1) - 1).astype(F32))
        counts.append(count.sum(-1))
    cols = jnp.stack([v[..., k] for v in (*ranks, gate) for k in range(top)], axis=1)
    return cols, jnp.stack(starts, axis=2), rows, jnp.maximum(*counts)


CAP = 576


def order(mb):
    r = [('r', k, k) for k in range(3)]
    c = [('c', m, m) for m in range(mb)]
    half = (mb + 2) // 2
    out = [('p', 0, 1), ('s', 1, 2)] + r[:1] + [('b', 0, 2), ('e', 0, 2), ('s', 2, mb)] + r[1:2] + c[:1] + r[2:]
    out += [('b', 2, half), ('b', half, mb), ('e', 2, mb)] + c[1:2]
    for m in range(mb):
        out += [('l', m, m)]
        if m + 2 < mb:
            out += c[m + 2:m + 3]
    return out


def solution(mesh):
    npp, nep = mesh.shape['pp'], mesh.shape['ep']
    over = [(i, (i + 1) % npp) for i in range(npp)]
    peer = [(i, (i + nep // 2) % nep) for i in range(nep)]
    sibling = [(i, i ^ 1) for i in range(nep)]
    tok_spec = P(('data', 'pp'), None, 'ep', None, None)
    wsp = P('pp', None, None, None)

    def body(O, idx, slot, g, H, w, Wq, Wk, Wv, Wo):
        o, h = O[0], H[0]
        mb, ne, cap, d = o.shape
        cg = cap // nep
        nt = h.shape[2]
        j = lax.axis_index('ep')
        x, c = j // 2, j % 2
        three = lambda a: a[0].reshape(mb, nt, a.shape[-1])
        cols, starts, rows, need = tables(three(idx), three(slot), three(g), x, c, j, ne, cg)
        send = jnp.stack([2 * x + 1 - c, (2 * x + 1 - c + 2) % nep]).astype(jnp.int32)
        fresh = jnp.zeros((8, 128), F32)
        wqkv = [a[0] for a in (Wq, Wk, Wv)]
        wo = Wo[0].reshape(d, d)

        full = 2 * ne * cg
        s0, tok = slice_rows(send, fresh, o, 0, 1, cg)
        d0 = lax.ppermute(s0, 'ep', sibling)
        tabs = [rows[NEAR], lax.ppermute(rows[FAR], 'ep', peer)]

        def run(tok, sib):
            over_cap = (need > CAP).astype(jnp.int32).max().reshape(1)
            for axis, pairs in (('ep', peer), ('pp', over), ('ep', sibling)):
                over_cap = jnp.maximum(over_cap, lax.ppermute(over_cap, axis, pairs))
            flags = jnp.broadcast_to(over_cap, (mb, 128 - starts[0].size))
            st = jnp.concatenate([starts.reshape(mb, -1), flags], axis=1).reshape(-1)
            near, far, packed, rest, ys = {}, {}, {}, {}, {}
            z = None

            def send_far(i, tok):
                v, tok = lax.optimization_barrier((packed.pop(i), tok))
                far[i] = lax.ppermute(v, 'ep', peer)
                return tok

            for kind, m, e in order(mb):
                if kind == 's':
                    s, tok = slice_rows(send, tok, o, m, e - m, cg)
                    s = lax.ppermute(s, 'ep', sibling)
                    for i in range(m, e):
                        sib[i] = (s, i - m)
                elif kind == 'r':
                    v, tok = lax.optimization_barrier((wqkv[m], tok))
                    wqkv[m], tok = lax.optimization_barrier((jnp.reshape(v, (d, d)), tok))
                elif kind in 'pb':
                    jobs = [(i, w_, 0, CAP) for i in range(m, e) for w_ in (FAR, NEAR)]
                    jobs = [b for b in jobs if (b[1] == FAR) == (kind == 'p') or b[0] > 0]
                    *out, tok = pack(tok, o, sib, tabs, jobs, cg)
                    for b, r in zip(jobs, out):
                        if b[1] == NEAR:
                            near[b[0]] = r
                        elif b[0] == 0:
                            far[0] = lax.ppermute(r, 'ep', peer)
                        else:
                            packed[b[0]] = r
                elif kind == 'e':
                    def more(tok):
                        past = [(i, w_, CAP, full - CAP) for w_ in (FAR, NEAR) for i in range(m, e)]
                        *out, tok = pack(tok, o, sib, tabs, past, cg)
                        return [lax.ppermute(v, 'ep', peer) for v in out[:e - m]] + out[e - m:] + [tok]

                    def none(tok):
                        return list(nothing(tok, [(full - CAP, d)] * (2 * (e - m))))

                    *out, tok = lax.cond(over_cap[0] > 0, more, none, tok)
                    rest.update({i: (out[e - m + k], out[k]) for k, i in enumerate(range(m, e))})
                    for i in sorted(packed)[:2]:
                        tok = send_far(i, tok)
                elif kind == 'c':
                    y, tok = combine(st, tok, h, near[m], far[m], *rest[m], cols, m, full)
                    ys[m] = [lax.ppermute(y, 'pp', over)]
                else:
                    z, tok = layer(ys[m], z, m, tok, w, *wqkv, wo, mb)
                    if m + 4 in packed:
                        tok = send_far(m + 4, tok)
            return z

        return run(tok, {0: (d0, 0)})[None]

    return jax.shard_map(body, mesh=mesh,
                         in_specs=(tok_spec, tok_spec, tok_spec, tok_spec, tok_spec, P('pp', None), wsp, wsp, wsp, wsp),
                         out_specs=tok_spec, check_vma=False)
```
